256 devices in a mesh: section: 8 (over x, core), row: 8 (over y, z_lo), col: 4 (over z_hi).
Axes of the slice: x: 4, y: 4, z: 8 (z_hi: 4, z_lo: 2; z = z_hi * 2 + z_lo), core: 2. Of those that a mesh axis runs over, the one named last changes fastest.
Arguments:
- tokens: bfloat16 [4096, 4096], P(('section', 'col'), 'row'), may hold values from -6 to 6
- grad_gate: bfloat16 [8, 8, 128, 14336], P('section', None, 'row', 'col'), may hold values from -0.5 to 0.5
- grad_up: bfloat16 [8, 8, 128, 14336], P('section', None, 'row', 'col'), may hold values from -0.5 to 0.5
- slot_token: int32 [8, 8, 128], P('section'), may hold values from 0 to 511, as said below
Outputs:
- gate_weight_grad: bfloat16 [8, 4096, 14336], P('section', 'row', 'col')
- up_weight_grad: bfloat16 [8, 4096, 14336], P('section', 'row', 'col')
The draws below stay inside these ranges and needn't reach their ends.
Inputs may be any that keep to these rules, and one draw needn't show every extreme that they name: slot_token[g, e, c] is a token of group g; every token of a group fills exactly two of its group's 8 * 128 slots, and every slot is filled.
All inputs are finite; a program needn't handle non-finite values.
Results may differ from the reference program's by a relative error of at most 0.001.
Values may be sent and summed in bfloat16 or wider, within the bound.
No kernel may reach another device: no remote copies, remote signals or barrier semaphores. Data moves between devices by JAX's collectives and lax.ppermute only.
A program may use at most 256 MiB of HBM per device.

```python
import jax
import jax.numpy as jnp
from jax import lax

D = 4096
FF = 14336
E = 8
TOK_SECTION = 512
CAP = 128
TOKENS = 4096
N_SECTION = 8


def draw_slot_token(key, part):

    def draw_group(group_id):
        shuffled = jax.random.permutation(jax.random.fold_in(key, group_id), 2 * TOK_SECTION)
        return (shuffled % TOK_SECTION).reshape(E, CAP)
    return jax.vmap(draw_group)(jnp.arange(TOKENS // TOK_SECTION)).astype(jnp.int32)


def block_levels(own_key, extent, shards, low, top_value):
    gain, own = 1.0, jax.random.fold_in(own_key, 6)
    for dim, blocks in shards:
        draws = jnp.exp(jax.random.uniform(jax.random.fold_in(own, dim), (blocks,), jnp.float32, low / len(shards), top_value / len(shards)))
        gain = gain * jnp.repeat(draws, extent[dim] // blocks).reshape([-1 if axis == dim else 1 for axis in range(len(extent))])
    return gain


def normal_values(rng, extent, width, most, pieces=(), held_as=jnp.bfloat16):
    array = jax.random.normal(rng, extent, jnp.float32) * width
    if len(pieces) > 0:
        array = block_levels(rng, extent, pieces, -0.22, 0.18) * array
    return jnp.clip(array, min=-most, max=most).astype(held_as)


def setup_inputs(seed: int = 0) -> dict:
    streams_of = jax.random.split(jax.random.key(seed), 5)
    return {
        "tokens": normal_values(streams_of[0], (TOKENS, D), 1.0, 6.0, ((0, 32), (1, 8))),
        "grad_gate": normal_values(streams_of[1], (N_SECTION, E, CAP, FF), ((2 * TOK_SECTION) ** -0.5), 0.5, ((0, 8), (2, 8), (3, 4))),
        "grad_up": normal_values(streams_of[2], (N_SECTION, E, CAP, FF), ((2 * TOK_SECTION) ** -0.5), 0.5, ((0, 8), (2, 8), (3, 4))),
        "slot_token": draw_slot_token(jax.random.fold_in(streams_of[4], 71), 0),
    }


def reference(tokens, grad_gate, grad_up, slot_token):
    groups = tokens.shape[0] // TOK_SECTION
    grouped = tokens.reshape(groups, TOK_SECTION, D)

    def one_expert(expert):
        chosen = slot_token[:, expert, :]
        picked = jax.vmap(lambda block, where: block[where])(grouped, chosen).astype(jnp.float32)
        gate_part = grad_gate[:, expert].astype(jnp.float32)
        up_part = grad_up[:, expert].astype(jnp.float32)
        gate_grad = jnp.einsum("gcd,gcf->df", picked, gate_part, precision=lax.Precision.HIGHEST)
        up_grad = jnp.einsum("gcd,gcf->df", picked, up_part, precision=lax.Precision.HIGHEST)
        return gate_grad.astype(jnp.bfloat16), up_grad.astype(jnp.bfloat16)

    gate_out, up_out = lax.map(one_expert, jnp.arange(E, dtype=jnp.int32))
    return gate_out, up_out
```

```python
import functools

import jax
import jax.numpy as jnp
from jax import lax
from jax.experimental import pallas as pl
from jax.experimental.pallas import tpu as pltpu
from jax.sharding import PartitionSpec as P


F = 3584
U = 16
BF = jnp.bfloat16


def move_x(a, k):
    return lax.ppermute(a, "section", [(s, (s + 2 * k) % 8) for s in range(8)])


def swap_core(a):
    return lax.ppermute(a, "section", [(s, s ^ 1) for s in range(8)])


def move_y(a, k):
    return lax.ppermute(a, "row", [(r, (r + 2 * k) % 8) for r in range(8)])


def swap_z(a):
    return lax.ppermute(a, "row", [(r, r ^ 1) for r in range(8)])


def move_col(a, k):
    return lax.ppermute(a, "col", [(c, (c + k) % 4) for c in range(4)])


ANY = pl.BlockSpec(memory_space=pl.ANY)


def copies(plan_of, n_copies, n_in, shapes):
    def kernel(*refs):
        ins, outs, sems = refs[:n_in], refs[n_in:-1], refs[-1]
        plan = plan_of(ins, outs)
        started = [pltpu.make_async_copy(s, d, sems.at[i]) for i, (s, d) in enumerate(plan)]
        for c in started:
            c.start()
        for c in started:
            c.wait()

    return pl.pallas_call(
        kernel,
        in_specs=[ANY] * n_in,
        out_specs=[ANY] * len(shapes),
        out_shape=[jax.ShapeDtypeStruct(s, BF) for s in shapes],
        scratch_shapes=[pltpu.SemaphoreType.DMA((n_copies,))],
    )


def units(ref, start, count=1):
    return ref.at[pl.ds(start * U, count * U), :]


def first_plan(ins, outs):
    gate, up = ins
    x1, x2, x3, sa = outs
    s = lax.axis_index("section")
    x, core = s // 2, s % 2
    plan = []
    for k, out in ((1, x1), (2, x2), (3, x3)):
        to = (x + k) % 4
        for cr, c in ((0, core), (1, 1 - core)):
            e = 2 * to + c
            plan += [(gate.at[e], units(out, 2 * cr)), (up.at[e], units(out, 2 * cr + 1))]
    e = 2 * x + 1 - core
    plan += [(gate.at[e], units(sa, 0)), (up.at[e], units(sa, 1))]
    return plan


def group_a_plan(ins, outs):
    gate, up, ra = ins
    (qa,) = outs
    e = lax.axis_index("section")
    return [
        (gate.at[e], units(qa, 0)),
        (units(ra, 0), units(qa, 1)),
        (up.at[e], units(qa, 2)),
        (units(ra, 1), units(qa, 3)),
    ]


def other_core_plan(ins, outs):
    return [(units(x, 2, 2), units(outs[0], 2 * k, 2)) for k, x in enumerate(ins)]


def group_b_plan(ins, outs):
    x1, x2, x3, rb = ins
    (qb,) = outs
    plan = []
    for i, x in enumerate((x1, x2, x3)):
        plan += [(units(x, 0), units(qb, 2 * i)), (units(rb, 2 * i), units(qb, 2 * i + 1))]
    for i, (x, j) in enumerate(((x2, 1), (x1, 0), (x3, 2))):
        plan += [(units(x, 1), units(qb, 6 + 2 * i)), (units(rb, 2 * j + 1), units(qb, 7 + 2 * i))]
    return plan


def gather_rows(q, nz, nh):
    a, b = nz * U, (nz + nh) * U
    qm = move_y(q, 1)
    qp = move_y(q, -1)
    qz = swap_z(q)
    d2 = qz[:a]
    d2m = move_y(d2, 1)
    d2p = move_y(d2, -1)
    yzm = swap_z(qm[a:])
    yzp = swap_z(qp[a:])
    f1 = move_y(qp[:b], -1)
    f2 = move_y(d2m, 1)
    f3 = move_y(qm[b:], 1)
    g1 = swap_z(f1[a:])
    g2 = swap_z(f3)
    pieces = [q, qz, qp, qm, d2p, yzp, d2m, yzm, f1, f3, f2, g1, g2]

    def at(j, i, u):
        h = 0 if u < nz else (1 if u < nz + nh else 2)
        if (j, i) == (0, 0):
            return 0, u
        if (j, i) == (0, 1):
            return 1, u
        if (j, i) == (1, 0):
            return 2, u
        if (j, i) == (3, 0):
            return 3, u
        if (j, i) == (1, 1):
            return (4, u) if h == 0 else (5, u - nz)
        if (j, i) == (3, 1):
            return (6, u) if h == 0 else (7, u - nz)
        if (j, i) == (2, 0):
            return (8, u) if h < 2 else (9, u - nz - nh)
        return (10, u) if h == 0 else ((11, u - nz) if h == 1 else (12, u - nz - nh))

    return pieces, at


def route_kernel(slot, t0, t1, t2, t3, o0, o1, o2, o3):
    s = lax.axis_index("section")
    row = lax.axis_index("row")
    col = lax.axis_index("col")
    x, core = s // 2, s % 2
    y, zl = row // 2, row % 2
    toks = slot[...]
    lane = lax.broadcasted_iota(jnp.int32, toks.shape, 1)
    toks = pltpu.roll(toks, (128 - 32 * y) % 128, 1)
    swapped = jnp.where((lane // 16) % 2 == 0, pltpu.roll(toks, 112, 1), pltpu.roll(toks, 16, 1))
    toks = jnp.where(zl == 0, toks, swapped)
    e_id = lax.broadcasted_iota(jnp.int32, toks.shape, 0)
    flipped = [t[...].T for t in (t0, t1, t2, t3)]
    source = jnp.concatenate(flipped, axis=1)
    tok = lax.broadcasted_iota(jnp.int32, (128, 128), 0)
    for k, out in enumerate((o0, o1, o2, o3)):
        for cr in range(2):
            c = core if cr == 0 else 1 - core
            e = 2 * ((x + k) % 4) + c
            mine = jnp.sum(jnp.where(e_id == e, toks, 0), axis=0, keepdims=True)
            hot = jnp.concatenate(
                [jnp.where(tok + 128 * ((col - j + 4) % 4) == mine, 1.0, 0.0).astype(BF) for j in range(4)], axis=0
            )
            out[cr] = jnp.dot(source, hot, preferred_element_type=jnp.float32).astype(BF)


def route(slot, toks):
    return pl.pallas_call(
        route_kernel,
        out_shape=[jax.ShapeDtypeStruct((2, 512, 128), BF)] * 4,
    )(slot, *toks)


def products(lhs, pieces, gate_at, up_at, tile=512):
    n = len(lhs)

    def kernel(*refs):
        a = jnp.concatenate([r[...] for r in refs[:n]], axis=1)
        ins = refs[n : n + len(pieces)]
        for where, out in ((gate_at, refs[-2]), (up_at, refs[-1])):
            b = jnp.concatenate([ins[p][u * U : (u + 1) * U, :] for p, u in where], axis=0)
            out[...] = jnp.dot(a, b, preferred_element_type=jnp.float32).astype(BF)

    return pl.pallas_call(
        kernel,
        grid=(F // tile,),
        in_specs=[pl.BlockSpec((512, 128), lambda j: (0, 0))] * n
        + [pl.BlockSpec((p.shape[0], tile), lambda j: (0, j)) for p in pieces],
        out_specs=[pl.BlockSpec((512, tile), lambda j: (0, j))] * 2,
        out_shape=[jax.ShapeDtypeStruct((512, F), BF)] * 2,
        compiler_params=pltpu.CompilerParams(vmem_limit_bytes=48 * 1024 * 1024),
    )(*lhs, *pieces)


def body(tokens, grad_gate, grad_up, slot_token):
    gate, up = grad_gate[0], grad_up[0]
    big = (4 * U, F)
    x1, x2, x3, sa = copies(first_plan, 14, 2, [big, big, big, (2 * U, F)])(gate, up)
    ra = swap_core(sa)
    r1, r3, r2 = move_x(x1, 1), move_x(x3, 3), move_x(x2, 2)
    toks = [tokens] + [move_col(tokens, k) for k in (1, 2, 3)]
    (qa,) = copies(group_a_plan, 4, 3, [big])(gate, up, ra)
    pieces_a, at_a = gather_rows(qa, 2, 1)
    (sb,) = copies(other_core_plan, 3, 3, [(6 * U, F)])(r1, r2, r3)
    rb = swap_core(sb)
    (qb,) = copies(group_b_plan, 12, 4, [(12 * U, F)])(r1, r2, r3, rb)
    pieces_b, at_b = gather_rows(qb, 8, 2)
    o0, o1, o2, o3 = route(slot_token[0], toks)
    a1, a3, a2 = move_x(o1, 1), move_x(o3, 3), move_x(o2, 2)
    held = [o0, a1, a2, a3]
    got = swap_core(jnp.stack([h[1] for h in held]))
    lhs = []
    for k in range(4):
        lhs += [held[k][0], got[k]]
    gate_at, up_at = [], []
    for k in range(4):
        for cr in range(2):
            for j in range(4):
                for i in range(2):
                    if k == 0:
                        for at, u in ((gate_at, cr), (up_at, 2 + cr)):
                            at.append(at_a(j, i, u))
                    else:
                        ug = 2 * (k - 1) + cr
                        uu = {2: 6, 1: 8, 3: 10}[k] + cr
                        for at, u in ((gate_at, ug), (up_at, uu)):
                            p, v = at_b(j, i, u)
                            at.append((p + len(pieces_a), v))
    g, u = products(lhs, pieces_a + pieces_b, gate_at, up_at)
    return g[None], u[None]


def solution(mesh):
    return jax.shard_map(
        body,
        mesh=mesh,
        in_specs=(
            P(("section", "col"), "row"),
            P("section", None, "row", "col"),
            P("section", None, "row", "col"),
            P("section", None, None),
        ),
        out_specs=(P("section", "row", "col"), P("section", "row", "col")),
        check_vma=False,
    )
```

```python
import jax
import jax.numpy as jnp
from jax import lax
from jax.experimental import pallas as pl
from jax.experimental.pallas import tpu as pltpu
from jax.sharding import PartitionSpec as P


F = 3584
U = 16
BF = jnp.bfloat16


def permute(a, axis, to, n):
    return lax.ppermute(a, axis, [(i, to(i)) for i in range(n)])


def move_x(a, k):
    return permute(a, "section", lambda s: (s + 2 * k) % 8, 8)


def swap_core(a):
    return permute(a, "section", lambda s: s ^ 1, 8)


def move_y(a, k):
    return permute(a, "row", lambda r: (r + 2 * k) % 8, 8)


def swap_z(a):
    return permute(a, "row", lambda r: r ^ 1, 8)


def move_col(a, k):
    return permute(a, "col", lambda c: (c + k) % 4, 4)


LIMIT = 24 * 1024 * 1024
IN_HBM = pl.BlockSpec(memory_space=pltpu.HBM)


def in_hbm(arrays):
    return [pltpu.with_memory_space_constraint(a, pltpu.HBM) for a in arrays]


def copies(plan_of, n_copies, ins, shapes):
    n_in = len(ins)

    def kernel(*refs):
        ins, outs, sems = refs[:n_in], refs[n_in:-1], refs[-1]
        plan = plan_of(ins, outs)
        started = [pltpu.make_async_copy(s, d, sems.at[i]) for i, (s, d) in enumerate(plan)]
        for c in started:
            c.start()
        for c in started:
            c.wait()

    return pl.pallas_call(
        kernel,
        in_specs=[IN_HBM] * n_in,
        out_shape=[jax.ShapeDtypeStruct(s, BF) for s in shapes],
        scratch_shapes=[pltpu.SemaphoreType.DMA((n_copies,))],
        compiler_params=pltpu.CompilerParams(vmem_limit_bytes=LIMIT),
    )(*in_hbm(ins))


def units(ref, start, count=1):
    return ref.at[pl.ds(start * U, count * U), :]


def first_plan(ins, outs):
    gate, up = ins
    x1, x2, x3, sa, oa = outs
    s = lax.axis_index("section")
    x, core = s // 2, s % 2
    plan = []
    for k, out in ((1, x1), (2, x2), (3, x3)):
        to = (x + k) % 4
        for cr, c in ((0, core), (1, 1 - core)):
            e = 2 * to + c
            plan += [(gate.at[e], units(out, 2 * cr)), (up.at[e], units(out, 2 * cr + 1))]
    for out, e in ((sa, 2 * x + 1 - core), (oa, s)):
        plan += [(gate.at[e], units(out, 0)), (up.at[e], units(out, 1))]
    return plan


def arrange(ins, outs):
    def kernel(*refs):
        for plan, out in zip(outs, refs[len(ins) :], strict=True):
            at = 0
            for n, first, count in plan:
                out[at * U : (at + count) * U, :] = refs[n][first * U : (first + count) * U, :]
                at += count

    return pl.pallas_call(
        kernel,
        out_shape=[jax.ShapeDtypeStruct((sum(c for _, _, c in plan) * U,) + ins[0].shape[1:], BF) for plan in outs],
        compiler_params=pltpu.CompilerParams(vmem_limit_bytes=LIMIT),
    )(*ins)


UNITS_B = [(0, k, c) for k in (1, 2, 3) for c in (0, 1)] + [(1, k, c) for k in (2, 1, 3) for c in (0, 1)]
NZ, NH = 8, 2


def group_b_units():
    return [(k - 1, w, 1) if c == 0 else (3, 2 * (k - 1) + w, 1) for w, k, c in UNITS_B]


def gather_merged(t, q, nz, nh):
    n = q.shape[0] // U
    qz = swap_z(q)
    qm = move_y(q, 1)
    qp = move_y(q, -1)
    (d2,) = arrange([qz], [[(0, 0, nz)]])
    d2m = move_y(d2, 1)
    d2p = move_y(d2, -1)
    yz, f1 = arrange([qm, qp], [[(0, nz, n - nz), (1, nz, n - nz)], [(1, 0, nz + nh)]])
    yz = swap_z(yz)
    f1 = move_y(f1, -1)
    (f2,) = arrange([d2m, qm], [[(0, 0, nz), (1, nz + nh, n - nz - nh)]])
    f2 = move_y(f2, 1)
    (g,) = arrange([f1, f2], [[(0, nz, nh), (1, nz, n - nz - nh)]])
    g = swap_z(g)
    pieces = {"q": q, "qz": qz, "qp": qp, "qm": qm, "d2p": d2p, "d2m": d2m, "yz": yz, "f1": f1, "f2": f2, "g": g}

    def at(j, i, u):
        whole = {(0, 0): "q", (0, 1): "qz", (1, 0): "qp", (3, 0): "qm"}
        if (j, i) in whole:
            return t + whole[j, i], u
        if (j, i) == (1, 1):
            return (t + "d2p", u) if u < nz else (t + "yz", n + u - 2 * nz)
        if (j, i) == (3, 1):
            return (t + "d2m", u) if u < nz else (t + "yz", u - nz)
        if i == 1:
            return (t + "f2", u) if u < nz else (t + "g", u - nz)
        return (t + "f1", u) if u < nz + nh else (t + "f2", u - nh)

    return {t + n: p for n, p in pieces.items()}, at


def gather_both(t, q, qz_z, qz_y, nz, nh):
    n = q.shape[0] // U
    d2 = swap_z(qz_z)
    qm = move_y(q, 1)
    qp = move_y(q, -1)
    qzy = swap_z(qz_y)
    d2m = move_y(d2, 1)
    d2p = move_y(d2, -1)
    yz, f1h, f3, f1z = arrange(
        [qm, qp], [[(0, nz, n - nz), (1, nz, n - nz)], [(1, nz, nh)], [(0, nz + nh, n - nz - nh)], [(1, 0, nz)]]
    )
    yz = swap_z(yz)
    f1h = move_y(f1h, -1)
    f3 = move_y(f3, 1)
    f1z = move_y(f1z, -1)
    f2 = move_y(d2m, 1)
    (g,) = arrange([f1h, f3], [[(0, 0, nh), (1, 0, n - nz - nh)]])
    g = swap_z(g)
    pieces = {"q": q, "d2": d2, "qzy": qzy, "qp": qp, "qm": qm, "d2p": d2p, "d2m": d2m, "yz": yz}
    pieces |= {"f1z": f1z, "f1h": f1h, "f3": f3, "f2": f2, "g": g}

    def at(j, i, u):
        whole = {(0, 0): "q", (1, 0): "qp", (3, 0): "qm"}
        if (j, i) in whole:
            return t + whole[j, i], u
        if (j, i) == (0, 1):
            return (t + "d2", u) if u < nz else (t + "qzy", u - nz)
        if (j, i) == (1, 1):
            return (t + "d2p", u) if u < nz else (t + "yz", n + u - 2 * nz)
        if (j, i) == (3, 1):
            return (t + "d2m", u) if u < nz else (t + "yz", u - nz)
        if i == 1:
            return (t + "f2", u) if u < nz else (t + "g", u - nz)
        if u < nz:
            return t + "f1z", u
        return (t + "f1h", u - nz) if u < nz + nh else (t + "f3", u - nz - nh)

    return {t + n: p for n, p in pieces.items()}, at


def route_kernel(slot, t0, t1, t2, t3, o0, o1, o2, o3):
    s = lax.axis_index("section")
    row = lax.axis_index("row")
    col = lax.axis_index("col")
    x, core = s // 2, s % 2
    y, zl = row // 2, row % 2
    toks = slot[...]
    lane = lax.broadcasted_iota(jnp.int32, toks.shape, 1)
    toks = pltpu.roll(toks, (128 - 32 * y) % 128, 1)
    swapped = jnp.where((lane // 16) % 2 == 0, pltpu.roll(toks, 112, 1), pltpu.roll(toks, 16, 1))
    toks = jnp.where(zl == 0, toks, swapped)
    e_id = lax.broadcasted_iota(jnp.int32, toks.shape, 0)
    source = jnp.concatenate([t[...] for t in (t0, t1, t2, t3)], axis=0)
    tok = lax.broadcasted_iota(jnp.int32, (128, 128), 0)
    for k, out in enumerate((o0, o1, o2, o3)):
        for cr in range(2):
            c = core if cr == 0 else 1 - core
            e = 2 * ((x + k) % 4) + c
            mine = jnp.sum(jnp.where(e_id == e, toks, 0), axis=0, keepdims=True)
            hot = jnp.concatenate(
                [jnp.where(tok + 128 * ((col - j + 4) % 4) == mine, 1.0, 0.0).T.astype(BF) for j in range(4)], axis=1
            )
            out[cr * 128 : (cr + 1) * 128, :] = jnp.dot(hot, source, preferred_element_type=jnp.float32).astype(BF)


def route(slot, toks):
    return pl.pallas_call(
        route_kernel,
        out_shape=[jax.ShapeDtypeStruct((256, 512), BF)] * 4,
        compiler_params=pltpu.CompilerParams(vmem_limit_bytes=LIMIT),
    )(slot, *toks)


def turned(held, got, orders):
    def kernel(*refs):
        for order, out in zip(orders, refs[5:], strict=True):
            rows = []
            for k, cr, j, i in order:
                ref, at = (refs[k], 0) if cr == 0 else (refs[4], 128 * k)
                at += 16 * (2 * j + i)
                rows.append(ref[at : at + 16, :])
            out[...] = jnp.concatenate(rows, axis=0).T

    return pl.pallas_call(
        kernel,
        out_shape=[jax.ShapeDtypeStruct((512, 16 * len(o)), BF) for o in orders],
        compiler_params=pltpu.CompilerParams(vmem_limit_bytes=LIMIT),
    )(*held, got)


def products(lhs, pieces, where, sums=None, tile=512):
    names = sorted({p for w in where for p, _ in w})
    arrays = [pieces[p] for p in names]
    n = len(arrays)
    extra = [] if sums is None else list(sums)

    m = 2 + n + len(extra)

    def kernel(*refs):
        lhs_refs, ins, old, outs, scratch = refs[:2], refs[2 : 2 + n], refs[2 + n : m], refs[m : m + 2], refs[m + 2 :]

        def product(i, at):
            b = jnp.concatenate([ins[names.index(p)][u * U : (u + 1) * U, at] for p, u in where[i]], axis=0)
            return jnp.dot(lhs_refs[i][...], b, preferred_element_type=jnp.float32)

        if extra:
            moves = []
            for j in range(F // tile):
                at = pl.ds(j * tile, tile)
                for i in range(2):
                    stage, sems = scratch[2 * i : 2 * i + 2]
                    stage[:, at] = (old[i][:, at] + product(i, at)).astype(BF)
                    moves.append(pltpu.make_async_copy(stage.at[:, at], outs[i].at[:, at], sems.at[j]))
                    moves[-1].start()
            for move in moves:
                move.wait()
        else:

            @pl.loop(0, F // tile)
            def _(j):
                at = pl.ds(pl.multiple_of(j * tile, tile), tile)
                for i in range(2):
                    outs[i][:, at] = product(i, at)

    k = sum(a.shape[1] for a in lhs)
    in_vmem = pl.BlockSpec(memory_space=pltpu.VMEM)
    return pl.pallas_call(
        kernel,
        in_specs=[in_vmem] * (2 + n + len(extra)),
        out_specs=[IN_HBM if extra else in_vmem] * 2,
        out_shape=[jax.ShapeDtypeStruct((512, F), BF) if extra else pltpu.VMEM((512, F), jnp.float32)] * 2,
        scratch_shapes=[pltpu.VMEM((512, F), BF), pltpu.SemaphoreType.DMA((F // tile,))] * (2 if extra else 0),
        cost_estimate=pl.CostEstimate(flops=2 * 512 * F * k, transcendentals=0, bytes_accessed=4 * 512 * F * 2),
        compiler_params=pltpu.CompilerParams(vmem_limit_bytes=LIMIT),
    )(*lhs, *[pltpu.with_memory_space_constraint(a, pltpu.VMEM) for a in arrays + extra])


def body(tokens, grad_gate, grad_up, slot_token):
    return step(tokens, grad_gate[0], grad_up[0], slot_token[0])


def step(tokens, gate, up, slot):
    big = (4 * U, F)
    x1, x2, x3, sa, oa = copies(first_plan, 16, [gate, up], [big] * 3 + [(2 * U, F)] * 2)
    ra = swap_core(sa)
    r1, r3, r2 = move_x(x1, 1), move_x(x3, 3), move_x(x2, 2)
    toks = [tokens] + [move_col(tokens, k) for k in (1, 2, 3)]
    (qa,) = arrange([oa, ra], [[(0, 0, 1), (1, 0, 1), (0, 1, 1), (1, 1, 1)]])
    pieces_a, at_a = gather_merged("a", qa, 2, 1)
    (sb,) = arrange([r1, r2, r3], [[(0, 2, 2), (1, 2, 2), (2, 2, 2)]])
    rb = swap_core(sb)
    u = group_b_units()
    qb, qbz, qby = arrange([r1, r2, r3, rb], [u, u[:NZ], u[NZ:]])
    pieces_b, at_b = gather_both("b", qb, qbz, qby, NZ, NH)
    o0, o1, o2, o3 = route(slot, toks)
    a1, a3, a2 = move_x(o1, 1), move_x(o3, 3), move_x(o2, 2)
    held = [o0, a1, a2, a3]
    (other,) = arrange(held, [[(n, 8, 8) for n in range(4)]])
    got = swap_core(other)
    late = {"bf1z", "bf2", "bg"}
    plan = [[[], []], [[], []]]
    for k in range(4):
        for cr in range(2):
            for j in range(4):
                for i in range(2):
                    for w in range(2):
                        p, v = at_a(j, i, 2 * w + cr) if k == 0 else at_b(j, i, UNITS_B.index((w, k, cr)))
                        plan[p in late][w].append(((k, cr, j, i), (p, v)))
    lhs = turned(held, got, [[o for o, _ in plan[n][w]] for n in range(2) for w in range(2)])
    pieces = pieces_a | pieces_b
    sums = None
    for n in range(2):
        where = [[at for _, at in plan[n][w]] for w in range(2)]
        sums = products(lhs[2 * n : 2 * n + 2], pieces, where, sums)
    return sums[0][None], sums[1][None]


def solution(mesh):
    return jax.shard_map(
        body,
        mesh=mesh,
        in_specs=(
            P(("section", "col"), "row"),
            P("section", None, "row", "col"),
            P("section", None, "row", "col"),
            P("section", None, None),
        ),
        out_specs=(P("section", "row", "col"), P("section", "row", "col")),
        check_vma=False,
    )
```

```python
import jax
import jax.numpy as jnp
from jax import lax
from jax.experimental import pallas as pl
from jax.experimental.pallas import tpu as pltpu
from jax.sharding import PartitionSpec as P


F = 3584
U = 16
BF = jnp.bfloat16


def permute(a, axis, to, n):
    return lax.ppermute(a, axis, [(i, to(i)) for i in range(n)])


def move_x(a, k):
    return permute(a, "section", lambda s: (s + 2 * k) % 8, 8)


def swap_core(a):
    return permute(a, "section", lambda s: s ^ 1, 8)


def move_y(a, k):
    return permute(a, "row", lambda r: (r + 2 * k) % 8, 8)


def swap_z(a):
    return permute(a, "row", lambda r: r ^ 1, 8)


def move_col(a, k):
    return permute(a, "col", lambda c: (c + k) % 4, 4)


LIMIT = 24 * 1024 * 1024
IN_HBM = pl.BlockSpec(memory_space=pltpu.HBM)


def in_hbm(arrays):
    return [pltpu.with_memory_space_constraint(a, pltpu.HBM) for a in arrays]


def copies(plan_of, n_copies, ins, shapes):
    n_in = len(ins)

    def kernel(*refs):
        ins, outs, sems = refs[:n_in], refs[n_in:-1], refs[-1]
        plan = plan_of(ins, outs)
        started = [pltpu.make_async_copy(s, d, sems.at[i]) for i, (s, d) in enumerate(plan)]
        for c in started:
            c.start()
        for c in started:
            c.wait()

    return pl.pallas_call(
        kernel,
        in_specs=[IN_HBM] * n_in,
        out_shape=[jax.ShapeDtypeStruct(s, BF) for s in shapes],
        scratch_shapes=[pltpu.SemaphoreType.DMA((n_copies,))],
        compiler_params=pltpu.CompilerParams(vmem_limit_bytes=LIMIT),
    )(*in_hbm(ins))


def units(ref, start, count=1):
    return ref.at[pl.ds(start * U, count * U), :]


def first_plan(ins, outs):
    gate, up = ins
    x1, x2, x3, sa, oa = outs
    s = lax.axis_index("section")
    x, core = s // 2, s % 2
    plan = []
    for k, out in ((1, x1), (2, x2), (3, x3)):
        to = (x + k) % 4
        for cr, c in ((0, core), (1, 1 - core)):
            e = 2 * to + c
            plan += [(gate.at[e], units(out, 2 * cr)), (up.at[e], units(out, 2 * cr + 1))]
    for out, e in ((sa, 2 * x + 1 - core), (oa, s)):
        plan += [(gate.at[e], units(out, 0)), (up.at[e], units(out, 1))]
    return plan


def arrange(ins, outs):
    width = ins[0].shape[1]
    plans = [o if isinstance(o, tuple) else (o, slice(0, width)) for o in outs]

    def kernel(*refs):
        for (plan, cols), out in zip(plans, refs[len(ins) :], strict=True):
            at = 0
            for n, first, count in plan:
                out[at * U : (at + count) * U, :] = refs[n][first * U : (first + count) * U, cols]
                at += count

    return pl.pallas_call(
        kernel,
        out_shape=[
            jax.ShapeDtypeStruct((sum(c for _, _, c in plan) * U, cols.stop - cols.start), BF) for plan, cols in plans
        ],
        compiler_params=pltpu.CompilerParams(vmem_limit_bytes=LIMIT),
    )(*ins)


UNITS_B = [(0, k, c) for k in (1, 2, 3) for c in (0, 1)] + [(1, k, c) for k in (2, 1, 3) for c in (0, 1)]
NZ, NH = 8, 2
PARTS = (slice(0, 1024), slice(1024, 2048), slice(2048, F))


def group_b_units():
    return [(k - 1, w, 1) if c == 0 else (3, 2 * (k - 1) + w, 1) for w, k, c in UNITS_B]


def gather_merged(t, q, nz, nh):
    n = q.shape[0] // U
    qz = swap_z(q)
    qm = move_y(q, 1)
    qp = move_y(q, -1)
    (d2,) = arrange([qz], [[(0, 0, nz)]])
    d2m = move_y(d2, 1)
    d2p = move_y(d2, -1)
    yz, f1 = arrange([qm, qp], [[(0, nz, n - nz), (1, nz, n - nz)], [(1, 0, nz + nh)]])
    yz = swap_z(yz)
    f1 = move_y(f1, -1)
    (f3,) = arrange([qm], [[(0, nz + nh, n - nz - nh)]])
    f3 = move_y(f3, 1)
    f2 = move_y(d2m, 1)
    (g,) = arrange([f1, f3], [[(0, nz, nh), (1, 0, n - nz - nh)]])
    g = swap_z(g)
    pieces = {"q": q, "qz": qz, "qp": qp, "qm": qm, "d2p": d2p, "d2m": d2m, "yz": yz}
    pieces |= {"f1": f1, "f2": f2, "f3": f3, "g": g}

    def at(j, i, u):
        whole = {(0, 0): "q", (0, 1): "qz", (1, 0): "qp", (3, 0): "qm"}
        if (j, i) in whole:
            return t + whole[j, i], u
        if (j, i) == (1, 1):
            return (t + "d2p", u) if u < nz else (t + "yz", n + u - 2 * nz)
        if (j, i) == (3, 1):
            return (t + "d2m", u) if u < nz else (t + "yz", u - nz)
        if i == 1:
            return (t + "f2", u) if u < nz else (t + "g", u - nz)
        return (t + "f1", u) if u < nz + nh else (t + "f3", u - nz - nh)

    return {t + n: p for n, p in pieces.items()}, at


def gather_both(t, q, qz_z, qz_y, nz, nh):
    n = q.shape[0] // U
    d2 = swap_z(qz_z)
    qm = move_y(q, 1)
    qp = move_y(q, -1)
    qzy = swap_z(qz_y)
    d2m = move_y(d2, 1)
    d2p = move_y(d2, -1)
    yz, f1h, f3, *f1z = arrange(
        [qm, qp],
        [[(0, nz, n - nz), (1, nz, n - nz)], [(1, nz, nh)], [(0, nz + nh, n - nz - nh)], *[([(1, 0, nz)], c) for c in PARTS]],
    )
    yz = swap_z(yz)
    f1h = move_y(f1h, -1)
    f3 = move_y(f3, 1)
    f1z = [move_y(f, -1) for f in f1z]
    f2 = arrange([d2m], [([(0, 0, nz)], c) for c in PARTS])
    f2 = [move_y(f, 1) for f in f2]
    g = arrange([f1h, f3], [([(0, 0, nh), (1, 0, n - nz - nh)], c) for c in PARTS])
    g = [swap_z(f) for f in g]
    pieces = {"q": q, "d2": d2, "qzy": qzy, "qp": qp, "qm": qm, "d2p": d2p, "d2m": d2m, "yz": yz}
    pieces |= {"f1z": f1z, "f1h": f1h, "f3": f3, "f2": f2, "g": g}

    def at(j, i, u):
        whole = {(0, 0): "q", (1, 0): "qp", (3, 0): "qm"}
        if (j, i) in whole:
            return t + whole[j, i], u
        if (j, i) == (0, 1):
            return (t + "d2", u) if u < nz else (t + "qzy", u - nz)
        if (j, i) == (1, 1):
            return (t + "d2p", u) if u < nz else (t + "yz", n + u - 2 * nz)
        if (j, i) == (3, 1):
            return (t + "d2m", u) if u < nz else (t + "yz", u - nz)
        if i == 1:
            return (t + "f2", u) if u < nz else (t + "g", u - nz)
        if u < nz:
            return t + "f1z", u
        return (t + "f1h", u - nz) if u < nz + nh else (t + "f3", u - nz - nh)

    return {t + n: p for n, p in pieces.items()}, at


def route_kernel(slot, t0, t1, t2, t3, o0, o1, o2, o3):
    s = lax.axis_index("section")
    row = lax.axis_index("row")
    col = lax.axis_index("col")
    x, core = s // 2, s % 2
    y, zl = row // 2, row % 2
    toks = slot[...]
    lane = lax.broadcasted_iota(jnp.int32, toks.shape, 1)
    toks = pltpu.roll(toks, (128 - 32 * y) % 128, 1)
    swapped = jnp.where((lane // 16) % 2 == 0, pltpu.roll(toks, 112, 1), pltpu.roll(toks, 16, 1))
    toks = jnp.where(zl == 0, toks, swapped)
    e_id = lax.broadcasted_iota(jnp.int32, toks.shape, 0)
    source = jnp.concatenate([t[...] for t in (t0, t1, t2, t3)], axis=0)
    tok = lax.broadcasted_iota(jnp.int32, (128, 128), 0)
    for k, out in enumerate((o0, o1, o2, o3)):
        for cr in range(2):
            c = core if cr == 0 else 1 - core
            e = 2 * ((x + k) % 4) + c
            mine = jnp.sum(jnp.where(e_id == e, toks, 0), axis=0, keepdims=True)
            hot = jnp.concatenate(
                [jnp.where(tok + 128 * ((col - j + 4) % 4) == mine, 1.0, 0.0).T.astype(BF) for j in range(4)], axis=1
            )
            out[cr * 128 : (cr + 1) * 128, :] = jnp.dot(hot, source, preferred_element_type=jnp.float32).astype(BF)


def route(slot, toks):
    return pl.pallas_call(
        route_kernel,
        out_shape=[jax.ShapeDtypeStruct((256, 512), BF)] * 4,
        compiler_params=pltpu.CompilerParams(vmem_limit_bytes=LIMIT),
    )(slot, *toks)


def turned(held, got, orders):
    def kernel(*refs):
        for order, out in zip(orders, refs[5:], strict=True):
            rows = []
            for k, cr, j, i in order:
                ref, at = (refs[k], 0) if cr == 0 else (refs[4], 128 * k)
                at += 16 * (2 * j + i)
                rows.append(ref[at : at + 16, :])
            out[...] = jnp.concatenate(rows, axis=0).T

    return pl.pallas_call(
        kernel,
        out_shape=[jax.ShapeDtypeStruct((512, 16 * len(o)), BF) for o in orders],
        compiler_params=pltpu.CompilerParams(vmem_limit_bytes=LIMIT),
    )(*held, got)


def products(lhs, pieces, where, sums=None, part=None, outs=(), tile=512):
    names = sorted({p for w in where for p, _ in w})
    split = [isinstance(pieces[p], list) for p in names]
    arrays = [pieces[p][part] if c else pieces[p] for p, c in zip(names, split, strict=True)]
    n = len(arrays)
    extra = [] if sums is None else list(sums)
    cols = slice(0, F) if part is None else PARTS[part]
    width = cols.stop - cols.start
    first = 2 + n + len(extra) + len(outs)

    def kernel(*refs):
        lhs_refs, ins, old = refs[:2], refs[2 : 2 + n], refs[2 + n : 2 + n + len(extra)]
        to, scratch = refs[first : first + 2], refs[first + 2 :]

        def product(i, at, own):
            rows = []
            for p, u in where[i]:
                m = names.index(p)
                rows.append(ins[m][u * U : (u + 1) * U, own if split[m] else at])
            return jnp.dot(lhs_refs[i][...], jnp.concatenate(rows, axis=0), preferred_element_type=jnp.float32)

        if extra:
            moves = []
            for j in range(width // tile):
                own, at = pl.ds(j * tile, tile), pl.ds(cols.start + j * tile, tile)
                for i in range(2):
                    stage, sems = scratch[2 * i : 2 * i + 2]
                    stage[:, own] = (old[i][:, at] + product(i, at, own)).astype(BF)
                    moves.append(pltpu.make_async_copy(stage.at[:, own], to[i].at[:, at], sems.at[j]))
                    moves[-1].start()
            for move in moves:
                move.wait()
        else:

            @pl.loop(0, F // tile)
            def _(j):
                at = pl.ds(pl.multiple_of(j * tile, tile), tile)
                for i in range(2):
                    to[i][:, at] = product(i, at, at)

    k = sum(a.shape[1] for a in lhs)
    in_vmem = pl.BlockSpec(memory_space=pltpu.VMEM)
    return pl.pallas_call(
        kernel,
        in_specs=[in_vmem] * (2 + n + len(extra)) + [IN_HBM] * len(outs),
        out_specs=[IN_HBM if extra else in_vmem] * 2,
        out_shape=[jax.ShapeDtypeStruct((512, F), BF) if extra else pltpu.VMEM((512, F), jnp.float32)] * 2,
        input_output_aliases={first - 2 + i: i for i in range(len(outs))},
        scratch_shapes=[pltpu.VMEM((512, width), BF), pltpu.SemaphoreType.DMA((width // tile,))] * (2 if extra else 0),
        cost_estimate=pl.CostEstimate(flops=1024 * width * k, transcendentals=0, bytes_accessed=4096 * width),
        compiler_params=pltpu.CompilerParams(vmem_limit_bytes=LIMIT),
    )(*lhs, *[pltpu.with_memory_space_constraint(a, pltpu.VMEM) for a in arrays + extra], *outs)


def body(tokens, grad_gate, grad_up, slot_token):
    return step(tokens, grad_gate[0], grad_up[0], slot_token[0])


def step(tokens, gate, up, slot):
    big = (4 * U, F)
    x1, x2, x3, sa, oa = copies(first_plan, 16, [gate, up], [big] * 3 + [(2 * U, F)] * 2)
    ra = swap_core(sa)
    r1, r3, r2 = move_x(x1, 1), move_x(x3, 3), move_x(x2, 2)
    toks = [tokens] + [move_col(tokens, k) for k in (1, 2, 3)]
    (qa,) = arrange([oa, ra], [[(0, 0, 1), (1, 0, 1), (0, 1, 1), (1, 1, 1)]])
    pieces_a, at_a = gather_merged("a", qa, 2, 1)
    (sb,) = arrange([r1, r2, r3], [[(0, 2, 2), (1, 2, 2), (2, 2, 2)]])
    rb = swap_core(sb)
    u = group_b_units()
    qb, qbz, qby = arrange([r1, r2, r3, rb], [u, u[:NZ], u[NZ:]])
    pieces_b, at_b = gather_both("b", qb, qbz, qby, NZ, NH)
    o0, o1, o2, o3 = route(slot, toks)
    a1, a3, a2 = move_x(o1, 1), move_x(o3, 3), move_x(o2, 2)
    held = [o0, a1, a2, a3]
    (other,) = arrange(held, [[(n, 8, 8) for n in range(4)]])
    got = swap_core(other)
    late = {"bf1z", "bf2", "bg", "byz"}
    plan = [[[], []], [[], []]]
    for k in range(4):
        for cr in range(2):
            for j in range(4):
                for i in range(2):
                    for w in range(2):
                        p, v = at_a(j, i, 2 * w + cr) if k == 0 else at_b(j, i, UNITS_B.index((w, k, cr)))
                        plan[p in late][w].append(((k, cr, j, i), (p, v)))
    lhs = turned(held, got, [[o for o, _ in plan[n][w]] for n in range(2) for w in range(2)])
    pieces = pieces_a | pieces_b
    where = [[[at for _, at in plan[n][w]] for w in range(2)] for n in range(2)]
    sums = products(lhs[:2], pieces, where[0])
    outs = ()
    for part in range(len(PARTS)):
        outs = products(lhs[2:], pieces, where[1], sums, part, outs)
    return outs[0][None], outs[1][None]


def solution(mesh):
    return jax.shard_map(
        body,
        mesh=mesh,
        in_specs=(
            P(("section", "col"), "row"),
            P("section", None, "row", "col"),
            P("section", None, "row", "col"),
            P("section", None, None),
        ),
        out_specs=(P("section", "row", "col"), P("section", "row", "col")),
        check_vma=False,
    )
```
